512 devices in a mesh: prow: 64 (over z, x, core), pcol: 8 (over y).
Axes of the slice: x: 4, y: 8, z: 8, core: 2. Of those that a mesh axis runs over, the one named last changes fastest.
Arguments:
- rhs: bfloat16 [3, 512, 128, 384], P(None, ('prow', 'pcol')), may hold values from -6 to 6
- inverses: bfloat16 [3, 512, 128, 128], P(None, ('prow', 'pcol')), may hold values from -0.16 to 1.5, as said below
- tiles_first: bfloat16 [64, 64, 8, 128, 128], P('prow', None, 'pcol'), may hold values from -0.0625 to 0.0625
- rows_first: int32 [64, 64, 8], P('prow', None, 'pcol'), may hold values from 0 to 15
- tiles_second: bfloat16 [64, 64, 8, 128, 128], P('prow', None, 'pcol'), may hold values from -0.0625 to 0.0625
- rows_second: int32 [64, 64, 8], P('prow', None, 'pcol'), may hold values from 0 to 7
Outputs:
- solved: bfloat16 [3, 512, 128, 384], P(None, ('prow', 'pcol'))
The draws below stay inside these ranges and needn't reach their ends.
Inputs may be any that keep to these rules, and one draw needn't show every extreme that they name: `inverses`: each block is lower triangular with its diagonal entries between 0.5 and 1.5.
All inputs are finite; a program needn't handle non-finite values.
Results may differ from the reference program's by a relative error of at most 0.0057.
Values may be sent and summed in bfloat16 or wider, within the bound.
No kernel may reach another device: no remote copies, remote signals or barrier semaphores. Data moves between devices by JAX's collectives and lax.ppermute only.
A program may use at most 128 MiB of HBM per device.

```python
import jax
import jax.numpy as jnp
from jax import lax

TILE = 128
RHS_COLS = 384
LEVELS = 3
BLOCKS = 512
N_PROW = 64
N_PCOL = 8


def draw_inverses(key, part):
    first_key, second_key = jax.random.split(jax.random.fold_in(key, 17))
    shape = (LEVELS, BLOCKS, TILE, TILE)
    diagonal = jax.random.uniform(first_key, (LEVELS, BLOCKS, TILE), jnp.float32, 0.5, 1.5)
    spread = 0.05 * jnp.clip(jax.random.normal(second_key, shape, jnp.float32), -3.0, 3.0)
    lower = jnp.tril(spread, -1)
    identity = jnp.eye(TILE, dtype=jnp.float32)
    full = lower + diagonal[..., None] * identity
    return full.astype(jnp.bfloat16)


def plant(values, own_key, smallest, top_value):
    place = [jax.random.randint(jax.random.fold_in(own_key, axis), (), 0, length) for axis, length in enumerate(values.shape)]
    longest = values.shape.index(max(values.shape))
    neighbour = place[:longest] + [(place[longest] + 1) % values.shape[longest]] + place[longest + 1:]
    return values.at[tuple(place)].set(smallest).at[tuple(neighbour)].set(top_value)


def shard_levels(rng, extent, pieces, low, largest):
    gain = 1.0
    for axis_at, shards_of in pieces:
        heights = jax.random.uniform(jax.random.fold_in(jax.random.fold_in(rng, 6), axis_at), (shards_of,), jnp.float32, low / len(pieces), largest / len(pieces))
        gain = gain * jnp.repeat(jnp.exp(heights), extent[axis_at] // shards_of).reshape((-1,) + (1,) * (len(extent) - 1 - axis_at))
    return gain


def scatter_about(rng, shape, deviation, reach, cuts=(), kind=jnp.bfloat16):
    loudness = shard_levels(rng, shape, cuts, -0.22, 0.18) if cuts else 1.0
    result = jax.random.normal(rng, shape, jnp.float32) * deviation * loudness
    return jnp.minimum(jnp.maximum(result, -reach), reach).astype(kind)


def setup_inputs(seed: int = 0) -> dict:
    seeds = jax.random.split(jax.random.key(seed), 7)
    rhs = scatter_about(seeds[0], (LEVELS, BLOCKS, TILE, RHS_COLS), 1.0, 6.0, ((1, 512),))
    inverses = draw_inverses(jax.random.fold_in(seeds[6], 71), 0)
    tiles_first = scatter_about(seeds[2], (N_PROW, N_PROW, N_PCOL, TILE, TILE), (TILE * N_PROW) ** -0.5, 0.0625, ((0, 64), (2, 8)))
    rows_first = plant(jax.random.randint(seeds[3], (N_PROW, N_PROW, N_PCOL), 0, 2 * N_PCOL), jax.random.fold_in(seeds[3], 1), 0, (2 * N_PCOL) - 1).astype(jnp.int32)
    tiles_second = scatter_about(seeds[4], (N_PROW, N_PROW, N_PCOL, TILE, TILE), (TILE * N_PROW) ** -0.5, 0.0625, ((0, 64), (2, 8)))
    rows_second = plant(jax.random.randint(seeds[5], (N_PROW, N_PROW, N_PCOL), 0, N_PCOL), jax.random.fold_in(seeds[5], 1), 0, N_PCOL - 1).astype(jnp.int32)
    return dict(rhs=rhs, inverses=inverses, tiles_first=tiles_first, rows_first=rows_first, tiles_second=tiles_second, rows_second=rows_second)


def apply_tiles(tiles, rows, level_solved, slots):
    width = level_solved.shape[-1]
    grid = level_solved.reshape(N_PROW, N_PCOL, TILE, width)

    def step(carry, column):
        tile = lax.dynamic_index_in_dim(tiles, column, 1, keepdims=False).astype(jnp.float32)
        block = lax.dynamic_index_in_dim(grid, column, 0, keepdims=False).astype(jnp.float32)
        product = jnp.einsum("pqab,qbr->pqar", tile, block, precision=lax.Precision.HIGHEST)
        which = lax.dynamic_index_in_dim(rows, column, 1, keepdims=False)
        onehot = (which[:, :, None] == jnp.arange(slots, dtype=jnp.int32)[None, None, :]).astype(jnp.float32)
        carry = carry + jnp.einsum("pqs,pqar->psar", onehot, product, precision=lax.Precision.HIGHEST)
        return carry, None

    init = jnp.zeros((N_PROW, slots, TILE, width), jnp.float32)
    total, _ = lax.scan(step, init, jnp.arange(N_PROW, dtype=jnp.int32))
    return total


def solve_blocks(inverse, reduced):
    right = reduced.astype(jnp.bfloat16)
    out = jnp.einsum("bij,bjr->bir", inverse.astype(jnp.float32), right.astype(jnp.float32), precision=lax.Precision.HIGHEST)
    return out.astype(jnp.bfloat16)


def reference(rhs, inverses, tiles_first, rows_first, tiles_second, rows_second):
    width = rhs.shape[-1]
    level_zero = solve_blocks(inverses[0], rhs[0].astype(jnp.float32))
    update_first = apply_tiles(tiles_first, rows_first, level_zero, 2 * N_PCOL)
    near = update_first[:, :N_PCOL].reshape(BLOCKS, TILE, width)
    level_one = solve_blocks(inverses[1], rhs[1].astype(jnp.float32) - near)
    update_second = apply_tiles(tiles_second, rows_second, level_one, N_PCOL)
    later = (update_first[:, N_PCOL:] + update_second).reshape(BLOCKS, TILE, width)
    level_two = solve_blocks(inverses[2], rhs[2].astype(jnp.float32) - later)
    return jnp.stack([level_zero, level_one, level_two])
```

```python
import functools

import jax
import jax.numpy as jnp
from jax import lax
from jax.experimental import pallas as pl
from jax.experimental.pallas import tpu as pltpu
from jax.sharding import Mesh, PartitionSpec as P


NZ, NX, NC, NY = 8, 4, 2, 8
TILE, COLS = 128, 384
HALF = NZ // 2
CHIPS = NZ * NX


def vmem():
    return pl.BlockSpec(memory_space=pltpu.VMEM)


def smem():
    return pl.BlockSpec(memory_space=pltpu.SMEM)


def solve_zero_body(inverse, right, out):
    out[...] = jnp.dot(inverse[...], right[...], preferred_element_type=jnp.float32).astype(jnp.bfloat16)


def solve_zero(inverse, right):
    return pl.pallas_call(
        solve_zero_body,
        out_shape=jax.ShapeDtypeStruct((TILE, COLS), jnp.bfloat16),
        in_specs=[vmem(), vmem()],
        out_specs=vmem(),
        cost_estimate=pl.CostEstimate(flops=2 * TILE * TILE * COLS, bytes_accessed=300000, transcendentals=0),
    )(inverse, right)


def solve_body(inverse, right, parts, out):
    total = parts[0].astype(jnp.float32)
    for q in range(1, NY):
        total = total + parts[q].astype(jnp.float32)
    reduced = (right[...].astype(jnp.float32) - total).astype(jnp.bfloat16)
    out[...] = jnp.dot(inverse[...], reduced, preferred_element_type=jnp.float32).astype(jnp.bfloat16)


def solve_next(inverse, right, parts):
    return pl.pallas_call(
        solve_body,
        out_shape=jax.ShapeDtypeStruct((TILE, COLS), jnp.bfloat16),
        in_specs=[vmem(), vmem(), vmem()],
        out_specs=vmem(),
        cost_estimate=pl.CostEstimate(flops=2 * TILE * TILE * COLS, bytes_accessed=1200000, transcendentals=0),
    )(inverse, right, parts)


def accumulate(rows, order, core, mine, other, pieces, acc):
    at = 0
    for piece in pieces:
        count = piece.shape[0]

        def step(j, carry, piece=piece, at=at):
            chip = order[at + j]
            block = piece[j]
            first = jnp.dot(mine[chip, core], block, preferred_element_type=jnp.float32)
            second = jnp.dot(other[chip], block, preferred_element_type=jnp.float32)
            acc[0, rows[0, chip]] += first
            acc[1, rows[1, chip]] += second
            return carry

        lax.fori_loop(0, count, step, 0, unroll=2)
        at += count


def first_body(rows, order, mine, other, *refs):
    pieces, near_mine, near_other, later, acc = refs[:7], refs[7], refs[8], refs[9], refs[10]
    acc[...] = jnp.zeros_like(acc)
    accumulate(rows, order, order[CHIPS], mine, other, pieces, acc)
    near_mine[...] = acc[0, :NY]
    near_other[...] = acc[1, :NY].astype(jnp.bfloat16)
    later[...] = acc[:, NY:]


def second_body(rows, order, mine, other, start, *refs):
    pieces, near_mine, near_other, acc = refs[:7], refs[7], refs[8], refs[9]
    acc[...] = start[...]
    accumulate(rows, order, order[CHIPS], mine, other, pieces, acc)
    near_mine[...] = acc[0]
    near_other[...] = acc[1].astype(jnp.bfloat16)


def spread(rows, order, mine, other, pieces, start=None):
    block = (NY, TILE, COLS)
    shapes = [jax.ShapeDtypeStruct(block, jnp.float32), jax.ShapeDtypeStruct(block, jnp.bfloat16)]
    operands = [rows, order, mine, other]
    if start is None:
        shapes.append(jax.ShapeDtypeStruct((2,) + block, jnp.float32))
        body, slots = first_body, 2 * NY
    else:
        operands.append(start)
        body, slots = second_body, NY
    return pl.pallas_call(
        body,
        out_shape=shapes,
        in_specs=[smem(), smem()] + [vmem()] * (len(operands) - 2 + len(pieces)),
        out_specs=[vmem()] * len(shapes),
        scratch_shapes=[pltpu.VMEM((2, slots, TILE, COLS), jnp.float32)],
        cost_estimate=pl.CostEstimate(flops=4 * CHIPS * TILE * TILE * COLS, bytes_accessed=12000000, transcendentals=0),
    )(*operands, *pieces)


def ring(n, d):
    return [(i, (i + d) % n) for i in range(n)]


def gather(block):
    up = functools.partial(lax.ppermute, axis_name="x", perm=ring(NX, 1))
    down = functools.partial(lax.ppermute, axis_name="x", perm=ring(NX, -1))
    own = lax.all_gather(block[None], "z", axis=0, tiled=True)
    low, high = own[:HALF], own[HALF:]
    low_left = up(low)
    high_right = down(high)
    high_left = up(high)
    low_right = down(low)
    low_far = up(low_left)
    high_far = down(high_right)
    return [own, low_left, high_right, high_left, low_right, low_far, high_far]


def chip_order():
    x = lax.axis_index("x")
    low = jnp.arange(HALF, dtype=jnp.int32) * NX
    high = low + HALF * NX
    left, right, far = (x + NX - 1) % NX, (x + 1) % NX, (x + 2) % NX
    core = lax.axis_index("core").astype(jnp.int32)[None]
    return jnp.concatenate([low + x, high + x, low + left, high + right, high + left, low + right, low + far, high + far, core]).astype(jnp.int32)


def swap(value):
    return lax.ppermute(value, "core", [(0, 1), (1, 0)])


def split_tiles(tiles, rows):
    core = lax.axis_index("core")
    mine = tiles[0, :, 0].reshape(CHIPS, NC, TILE, TILE)
    other = swap(lax.dynamic_index_in_dim(mine, 1 - core, 1, keepdims=False))
    slots = rows[0, :, 0].reshape(CHIPS, NC)
    own_slots = lax.dynamic_index_in_dim(slots, core, 1, keepdims=False)
    other_slots = swap(lax.dynamic_index_in_dim(slots, 1 - core, 1, keepdims=False))
    return mine, other, jnp.stack([own_slots, other_slots])


def reduce_rows(near_mine, near_other):
    total = near_mine + swap(near_other).astype(jnp.float32)
    return lax.all_to_all(total.astype(jnp.bfloat16), "y", 0, 0, tiled=True)


def local(rhs, inverses, tiles_first, rows_first, tiles_second, rows_second):
    order = chip_order()
    level_zero = solve_zero(inverses[0, 0], rhs[0, 0])
    first = split_tiles(tiles_first, rows_first)
    second = split_tiles(tiles_second, rows_second)

    pieces = gather(level_zero)
    near_mine, near_other, later = spread(first[2], order, first[0], first[1], pieces)
    level_one = solve_next(inverses[1, 0], rhs[1, 0], reduce_rows(near_mine, near_other))

    pieces = gather(level_one)
    near_mine, near_other = spread(second[2], order, second[0], second[1], pieces, later)
    level_two = solve_next(inverses[2, 0], rhs[2, 0], reduce_rows(near_mine, near_other))
    return jnp.stack([level_zero, level_one, level_two])[:, None]


def solution(mesh):
    grid = Mesh(mesh.devices.reshape(NZ, NX, NC, NY), ("z", "x", "core", "y"))
    blocks = ("z", "x", "core", "y")
    rows = ("z", "x", "core")
    in_specs = (
        P(None, blocks, None, None),
        P(None, blocks, None, None),
        P(rows, None, "y", None, None),
        P(rows, None, "y"),
        P(rows, None, "y", None, None),
        P(rows, None, "y"),
    )
    out_specs = P(None, blocks, None, None)
    return jax.shard_map(local, mesh=grid, in_specs=in_specs, out_specs=out_specs, check_vma=False)
```

```python
import functools

import jax
import jax.numpy as jnp
from jax import lax
from jax.experimental import pallas as pl
from jax.experimental.pallas import tpu as pltpu
from jax.sharding import Mesh, PartitionSpec as P


NZ, NX, NC, NY = 8, 4, 2, 8
TILE, COLS = 128, 384
HALF = NZ // 2
CHIPS = NZ * NX
NEAR_SPOTS = ((0, 0), (0, 1), (HALF, 2), (HALF, 1), (0, 2))
FAR_SPOTS = ((0, 3), (HALF, 3))
SOLVE_FLOPS = 2 * TILE * TILE * COLS
PAIR_FLOPS = 2 * SOLVE_FLOPS


MIB = 1 << 20


def vmem():
    return pl.BlockSpec(memory_space=pltpu.VMEM)


def smem():
    return pl.BlockSpec(memory_space=pltpu.SMEM)


def call(body, out_shape, in_specs, out_specs, operands, flops, limit, aliases=None, grid_spec=None):
    specs = {} if grid_spec is not None else {"in_specs": in_specs, "out_specs": out_specs}
    if grid_spec is not None:
        specs = {"grid_spec": grid_spec}
    return pl.pallas_call(
        body,
        out_shape=out_shape,
        input_output_aliases=aliases or {},
        compiler_params=pltpu.CompilerParams(vmem_limit_bytes=limit * MIB),
        cost_estimate=pl.CostEstimate(flops=flops, bytes_accessed=4 * MIB, transcendentals=0),
        **specs,
    )(*operands)


def block_shape(dtype, *lead):
    return jax.ShapeDtypeStruct(lead + (TILE, COLS), dtype)


def level_specs(level):
    return [
        pl.BlockSpec((1, 1, TILE, TILE), lambda i: (level, 0, 0, 0)),
        pl.BlockSpec((1, 1, TILE, COLS), lambda i: (level, 0, 0, 0)),
    ]


def solve_zero_body(inverse, right, out):
    out[...] = jnp.dot(inverse[0, 0], right[0, 0], preferred_element_type=jnp.float32).astype(jnp.bfloat16)


def solve_zero(inverses, rhs):
    grid_spec = pl.GridSpec(grid=(1,), in_specs=level_specs(0), out_specs=pl.BlockSpec((TILE, COLS), lambda i: (0, 0)))
    return call(solve_zero_body, block_shape(jnp.bfloat16), None, None, (inverses, rhs), SOLVE_FLOPS, 8, grid_spec=grid_spec)


def solve_body(inverse, right, parts, out):
    total = parts[0].astype(jnp.float32)
    for q in range(1, NY):
        total = total + parts[q].astype(jnp.float32)
    reduced = (right[0, 0].astype(jnp.float32) - total).astype(jnp.bfloat16)
    out[...] = jnp.dot(inverse[0, 0], reduced, preferred_element_type=jnp.float32).astype(jnp.bfloat16)


def solve_next(level, inverses, rhs, parts):
    grid_spec = pl.GridSpec(
        grid=(1,),
        in_specs=level_specs(level) + [pl.BlockSpec((NY, TILE, COLS), lambda i: (0, 0, 0))],
        out_specs=pl.BlockSpec((TILE, COLS), lambda i: (0, 0)),
    )
    return call(solve_body, block_shape(jnp.bfloat16), None, None, (inverses, rhs, parts), SOLVE_FLOPS, 8, grid_spec=grid_spec)


def accumulate(where, slots, received, level, mine, other, pieces, spots, state):
    core = where[NX]
    for piece, (base, side) in zip(pieces, spots):

        def step(j, carry, piece=piece, base=base, side=side):
            chip = (base + j) * NX + where[side]
            pair = jnp.concatenate([mine[chip, core], other[level, chip]], axis=0)
            product = jnp.dot(pair, piece[j], preferred_element_type=jnp.float32)
            state[0, slots[level, chip * NC + core]] += product[:TILE]
            state[1, received[level, chip * NC + core]] += product[TILE:]
            return carry

        lax.fori_loop(0, piece.shape[0], step, 0, unroll=4)


def early_first_body(where, slots, received, mine, other, *refs):
    pieces, state = refs[:-1], refs[-1]
    state[...] = jnp.zeros_like(state)
    accumulate(where, slots, received, 0, mine, other, pieces, NEAR_SPOTS, state)


def early_second_body(where, slots, received, mine, other, later, *refs):
    pieces, state = refs[:-1], refs[-1]
    state[...] = later[:, NY:]
    accumulate(where, slots, received, 1, mine, other, pieces, NEAR_SPOTS, state)


def early(tables, mine, other, pieces, later=None):
    operands = tables + (mine, other) + (() if later is None else (later,)) + tuple(pieces)
    return call(
        early_first_body if later is None else early_second_body,
        block_shape(jnp.float32, 2, 2 * NY if later is None else NY),
        [smem()] * 3 + [vmem()] * (len(operands) - 3),
        vmem(),
        operands,
        24 * PAIR_FLOPS,
        28,
    )


def late_body(level, where, slots, received, mine, other, state, low, high, out, near_other):
    del state
    accumulate(where, slots, received, level, mine, other, (low, high), FAR_SPOTS, out)
    near_other[...] = out[1, :NY].astype(jnp.bfloat16)


def late(level, tables, mine, other, state, pieces):
    return call(
        functools.partial(late_body, level),
        [jax.ShapeDtypeStruct(state.shape, jnp.float32), block_shape(jnp.bfloat16, NY)],
        [smem()] * 3 + [vmem()] * 5,
        [vmem()] * 2,
        tables + (mine, other, state) + tuple(pieces),
        8 * PAIR_FLOPS,
        28,
        aliases={5: 0},
    )


def join_body(state, received, out):
    out[...] = (state[0] + received[...].astype(jnp.float32)).astype(jnp.bfloat16)


def join(state, received):
    grid_spec = pl.GridSpec(
        grid=(1,),
        in_specs=[
            pl.BlockSpec((1, NY, TILE, COLS), lambda i: (0, 0, 0, 0)),
            pl.BlockSpec((NY, TILE, COLS), lambda i: (0, 0, 0)),
        ],
        out_specs=pl.BlockSpec((NY, TILE, COLS), lambda i: (0, 0, 0)),
    )
    return call(join_body, block_shape(jnp.bfloat16, NY), None, None, (state, received), SOLVE_FLOPS, 12, grid_spec=grid_spec)


def ring(n, d):
    return [(i, (i + d) % n) for i in range(n)]


def gather_rows(block):
    return lax.all_gather(block[None], "z", axis=0, tiled=True)


def gather_columns(own):
    up = functools.partial(lax.ppermute, axis_name="x", perm=ring(NX, 1))
    down = functools.partial(lax.ppermute, axis_name="x", perm=ring(NX, -1))
    low, high = own[:HALF], own[HALF:]
    low_left = up(low)
    high_right = down(high)
    high_left = up(high)
    low_right = down(low)
    low_far = up(low_left)
    high_far = down(high_right)
    return [own, low_left, high_right, high_left, low_right], [low_far, high_far]


def places():
    x = lax.axis_index("x")
    core = lax.axis_index("core")
    return jnp.stack([x, (x + NX - 1) % NX, (x + 1) % NX, (x + 2) % NX, core]).astype(jnp.int32)


def swap(value):
    return lax.ppermute(value, "core", [(0, 1), (1, 0)])


def pick_body(other, first, second, after, out):
    del other, after
    out[0] = first[:, 0]
    out[1] = second[:, 0]


def pick(first, second, after):
    half = (CHIPS, 1, TILE, TILE)
    grid_spec = pltpu.PrefetchScalarGridSpec(
        num_scalar_prefetch=1,
        grid=(1,),
        in_specs=[
            pl.BlockSpec(half, lambda i, other: (0, other[0], 0, 0)),
            pl.BlockSpec(half, lambda i, other: (0, other[0], 0, 0)),
            pl.BlockSpec(memory_space=pl.ANY),
        ],
        out_specs=pl.BlockSpec((2, CHIPS, TILE, TILE), lambda i, other: (0, 0, 0, 0)),
    )
    shape = jax.ShapeDtypeStruct((2, CHIPS, TILE, TILE), jnp.bfloat16)
    other = (1 - lax.axis_index("core")).astype(jnp.int32)[None]
    return call(pick_body, shape, None, None, (other, first, second, after), SOLVE_FLOPS, 12, grid_spec=grid_spec)


def reduce_rows(state, near_other):
    received = swap(near_other)
    return lax.all_to_all(join(state, received), "y", 0, 0, tiled=True)


def local(rhs, inverses, tiles_first, rows_first, tiles_second, rows_second):
    where = places()
    mine_first = tiles_first.reshape(CHIPS, NC, TILE, TILE)
    mine_second = tiles_second.reshape(CHIPS, NC, TILE, TILE)

    level_zero = solve_zero(inverses, rhs)
    own = gather_rows(level_zero)
    near, far = gather_columns(own)
    slots = jnp.concatenate([rows_first.reshape(1, CHIPS * NC), rows_second.reshape(1, CHIPS * NC)])
    received = swap(slots)
    others = swap(pick(mine_first, mine_second, own))
    tables = (where, slots, received)
    state = early(tables, mine_first, others, near)
    state, near_other = late(0, tables, mine_first, others, state, far)
    parts = reduce_rows(state, near_other)

    level_one = solve_next(1, inverses, rhs, parts)
    near, far = gather_columns(gather_rows(level_one))
    state = early(tables, mine_second, others, near, state)
    state, near_other = late(1, tables, mine_second, others, state, far)
    level_two = solve_next(2, inverses, rhs, reduce_rows(state, near_other))
    return jnp.stack([level_zero, level_one, level_two])[:, None]


def solution(mesh):
    grid = Mesh(mesh.devices.reshape(NZ, NX, NC, NY), ("z", "x", "core", "y"))
    blocks = ("z", "x", "core", "y")
    rows = ("z", "x", "core")
    in_specs = (
        P(None, blocks, None, None),
        P(None, blocks, None, None),
        P(rows, None, "y", None, None),
        P(rows, None, "y"),
        P(rows, None, "y", None, None),
        P(rows, None, "y"),
    )
    out_specs = P(None, blocks, None, None)
    return jax.shard_map(local, mesh=grid, in_specs=in_specs, out_specs=out_specs, check_vma=False)
```

```python
import functools

import jax
import jax.numpy as jnp
from jax import lax
from jax.experimental import pallas as pl
from jax.experimental.pallas import tpu as pltpu
from jax.sharding import Mesh, PartitionSpec as P


NQ, NP, NX, NC, NY = 4, 2, 4, 2, 8
TILE, COLS = 128, 384
CHIPS = NQ * NP * NX
NEAR_SPOTS = ((0, 0), (1, 0), (0, 1), (1, 2), (1, 1), (0, 2))
FAR_SPOTS = ((0, 3), (1, 3))
SOLVE_FLOPS = 2 * TILE * TILE * COLS
PAIR_FLOPS = 2 * SOLVE_FLOPS


MIB = 1 << 20


def vmem():
    return pl.BlockSpec(memory_space=pltpu.VMEM)


def smem():
    return pl.BlockSpec(memory_space=pltpu.SMEM)


def call(body, out_shape, in_specs, out_specs, operands, flops, limit, aliases=None, grid_spec=None):
    specs = {} if grid_spec is not None else {"in_specs": in_specs, "out_specs": out_specs}
    if grid_spec is not None:
        specs = {"grid_spec": grid_spec}
    return pl.pallas_call(
        body,
        out_shape=out_shape,
        input_output_aliases=aliases or {},
        compiler_params=pltpu.CompilerParams(vmem_limit_bytes=limit * MIB),
        cost_estimate=pl.CostEstimate(flops=flops, bytes_accessed=4 * MIB, transcendentals=0),
        **specs,
    )(*operands)


def block_shape(dtype, *lead):
    return jax.ShapeDtypeStruct(lead + (TILE, COLS), dtype)


def level_specs(level):
    return [
        pl.BlockSpec((1, 1, TILE, TILE), lambda i: (level, 0, 0, 0)),
        pl.BlockSpec((1, 1, TILE, COLS), lambda i: (level, 0, 0, 0)),
    ]


def solve_zero_body(inverse, right, out):
    out[...] = jnp.dot(inverse[0, 0], right[0, 0], preferred_element_type=jnp.float32).astype(jnp.bfloat16)


def solve_zero(inverses, rhs):
    grid_spec = pl.GridSpec(grid=(1,), in_specs=level_specs(0), out_specs=pl.BlockSpec((TILE, COLS), lambda i: (0, 0)))
    return call(solve_zero_body, block_shape(jnp.bfloat16), None, None, (inverses, rhs), SOLVE_FLOPS, 8, grid_spec=grid_spec)


def solve_body(inverse, right, parts, out):
    total = parts[0].astype(jnp.float32)
    for q in range(1, NY):
        total = total + parts[q].astype(jnp.float32)
    reduced = (right[0, 0].astype(jnp.float32) - total).astype(jnp.bfloat16)
    out[...] = jnp.dot(inverse[0, 0], reduced, preferred_element_type=jnp.float32).astype(jnp.bfloat16)


def solve_next(level, inverses, rhs, parts):
    grid_spec = pl.GridSpec(
        grid=(1,),
        in_specs=level_specs(level) + [pl.BlockSpec((NY, TILE, COLS), lambda i: (0, 0, 0))],
        out_specs=pl.BlockSpec((TILE, COLS), lambda i: (0, 0)),
    )
    return call(solve_body, block_shape(jnp.bfloat16), None, None, (inverses, rhs, parts), SOLVE_FLOPS, 8, grid_spec=grid_spec)


def accumulate(where, slots, received, level, mine, other, pieces, spots, state):
    core = where[NX]
    for piece, (base, side) in zip(pieces, spots):

        def step(j, carry, piece=piece, base=base, side=side):
            chip = (base + 2 * j) * NX + where[side]
            pair = jnp.concatenate([mine[chip, core], other[chip, core]], axis=0)
            product = jnp.dot(pair, piece[j], preferred_element_type=jnp.float32)
            state[0, slots[level, chip * NC + core]] += product[:TILE]
            state[1, received[level, chip * NC + core]] += product[TILE:]
            return carry

        lax.fori_loop(0, piece.shape[0], step, 0, unroll=4)


def early_first_body(where, slots, received, mine, other, *refs):
    pieces, state = refs[:-1], refs[-1]
    state[...] = jnp.zeros_like(state)
    accumulate(where, slots, received, 0, mine, other, pieces, NEAR_SPOTS, state)


def early_second_body(where, slots, received, mine, other, later, *refs):
    pieces, state = refs[:-1], refs[-1]
    state[...] = later[:, NY:]
    accumulate(where, slots, received, 1, mine, other, pieces, NEAR_SPOTS, state)


def early(tables, mine, other, pieces, later=None):
    operands = tables + (mine, other) + (() if later is None else (later,)) + tuple(pieces)
    return call(
        early_first_body if later is None else early_second_body,
        block_shape(jnp.float32, 2, 2 * NY if later is None else NY),
        [smem()] * 3 + [vmem()] * (len(operands) - 3),
        vmem(),
        operands,
        24 * PAIR_FLOPS,
        28,
    )


def late_body(level, where, slots, received, mine, other, state, low, high, out, near_other):
    del state
    accumulate(where, slots, received, level, mine, other, (low, high), FAR_SPOTS, out)
    near_other[...] = out[1, :NY].astype(jnp.bfloat16)


def late(level, tables, mine, other, state, pieces):
    return call(
        functools.partial(late_body, level),
        [jax.ShapeDtypeStruct(state.shape, jnp.float32), block_shape(jnp.bfloat16, NY)],
        [smem()] * 3 + [vmem()] * 5,
        [vmem()] * 2,
        tables + (mine, other, state) + tuple(pieces),
        8 * PAIR_FLOPS,
        28,
        aliases={5: 0},
    )


def join_body(state, received, out):
    out[...] = (state[0] + received[...].astype(jnp.float32)).astype(jnp.bfloat16)


def join(state, received):
    grid_spec = pl.GridSpec(
        grid=(1,),
        in_specs=[
            pl.BlockSpec((1, NY, TILE, COLS), lambda i: (0, 0, 0, 0)),
            pl.BlockSpec((NY, TILE, COLS), lambda i: (0, 0, 0)),
        ],
        out_specs=pl.BlockSpec((NY, TILE, COLS), lambda i: (0, 0, 0)),
    )
    return call(join_body, block_shape(jnp.bfloat16, NY), None, None, (state, received), SOLVE_FLOPS, 12, grid_spec=grid_spec)


def ring(n, d):
    return [(i, (i + d) % n) for i in range(n)]


def gather_rows(block):
    even_odd = lax.all_gather(block[None], "zq", axis=0, tiled=True)
    return lax.all_gather(even_odd[None], "zp", axis=0, tiled=True)


def gather_columns(own):
    up = functools.partial(lax.ppermute, axis_name="x", perm=ring(NX, 1))
    down = functools.partial(lax.ppermute, axis_name="x", perm=ring(NX, -1))
    low, high = own[0], own[1]
    low_left = up(low)
    high_right = down(high)
    high_left = up(high)
    low_right = down(low)
    low_far = up(low_left)
    high_far = down(high_right)
    return [low, high, low_left, high_right, high_left, low_right], [low_far, high_far]


def places():
    x = lax.axis_index("x")
    core = lax.axis_index("core")
    return jnp.stack([x, (x + NX - 1) % NX, (x + 1) % NX, (x + 2) % NX, core]).astype(jnp.int32)


def swap(value):
    return lax.ppermute(value, "core", [(0, 1), (1, 0)])


def reduce_rows(state, near_other):
    received = swap(near_other)
    return lax.all_to_all(join(state, received), "y", 0, 0, tiled=True)


def local(rhs, inverses, tiles_first, rows_first, tiles_second, rows_second):
    where = places()
    mine_first = tiles_first.reshape(CHIPS, NC, TILE, TILE)
    mine_second = tiles_second.reshape(CHIPS, NC, TILE, TILE)

    others = swap(mine_first)
    level_zero = solve_zero(inverses, rhs)
    near, far = gather_columns(gather_rows(level_zero))
    slots = jnp.concatenate([rows_first.reshape(1, CHIPS * NC), rows_second.reshape(1, CHIPS * NC)])
    received = swap(slots)
    tables = (where, slots, received)
    state = early(tables, mine_first, others, near)
    state, near_other = late(0, tables, mine_first, others, state, far)
    parts = reduce_rows(state, near_other)

    level_one = solve_next(1, inverses, rhs, parts)
    near, far = gather_columns(gather_rows(level_one))
    others = swap(mine_second)
    state = early(tables, mine_second, others, near, state)
    state, near_other = late(1, tables, mine_second, others, state, far)
    level_two = solve_next(2, inverses, rhs, reduce_rows(state, near_other))
    return jnp.stack([level_zero, level_one, level_two])[:, None]


def solution(mesh):
    grid = Mesh(mesh.devices.reshape(NQ, NP, NX, NC, NY), ("zq", "zp", "x", "core", "y"))
    blocks = ("zq", "zp", "x", "core", "y")
    rows = ("zq", "zp", "x", "core")
    in_specs = (
        P(None, blocks, None, None),
        P(None, blocks, None, None),
        P(rows, None, "y", None, None),
        P(rows, None, "y"),
        P(rows, None, "y", None, None),
        P(rows, None, "y"),
    )
    out_specs = P(None, blocks, None, None)
    return jax.shard_map(local, mesh=grid, in_specs=in_specs, out_specs=out_specs, check_vma=False)
```

```python
import functools

import jax
import jax.numpy as jnp
from jax import lax
from jax.experimental import pallas as pl
from jax.experimental.pallas import tpu as pltpu
from jax.sharding import Mesh, PartitionSpec as P


NQ, NP, NX, NC, NY = 4, 2, 4, 2, 8
TILE, COLS = 128, 384
CHIPS = NQ * NP * NX
NEAR_SPOTS = ((0, 0), (1, 0), (0, 1), (1, 2), (1, 1), (0, 2))
FAR_SPOTS = ((0, 3), (1, 3))
SOLVE_FLOPS = 2 * TILE * TILE * COLS
PAIR_FLOPS = 2 * SOLVE_FLOPS


MIB = 1 << 20


def vmem():
    return pl.BlockSpec(memory_space=pltpu.VMEM)


def smem():
    return pl.BlockSpec(memory_space=pltpu.SMEM)


def call(body, out_shape, in_specs, out_specs, operands, flops, limit, aliases=None, grid_spec=None):
    specs = {} if grid_spec is not None else {"in_specs": in_specs, "out_specs": out_specs}
    if grid_spec is not None:
        specs = {"grid_spec": grid_spec}
    return pl.pallas_call(
        body,
        out_shape=out_shape,
        input_output_aliases=aliases or {},
        compiler_params=pltpu.CompilerParams(vmem_limit_bytes=limit * MIB),
        cost_estimate=pl.CostEstimate(flops=flops, bytes_accessed=4 * MIB, transcendentals=0),
        **specs,
    )(*operands)


def block_shape(dtype, *lead):
    return jax.ShapeDtypeStruct(lead + (TILE, COLS), dtype)


def level_specs(level):
    return [
        pl.BlockSpec((1, 1, TILE, TILE), lambda i: (level, 0, 0, 0)),
        pl.BlockSpec((1, 1, TILE, COLS), lambda i: (level, 0, 0, 0)),
    ]


def solve_zero_body(inverse, right, out):
    out[...] = jnp.dot(inverse[0, 0], right[0, 0], preferred_element_type=jnp.float32).astype(jnp.bfloat16)


def solve_zero(inverses, rhs):
    grid_spec = pl.GridSpec(grid=(1,), in_specs=level_specs(0), out_specs=pl.BlockSpec((TILE, COLS), lambda i: (0, 0)))
    return call(solve_zero_body, block_shape(jnp.bfloat16), None, None, (inverses, rhs), SOLVE_FLOPS, 60, grid_spec=grid_spec)


def solve_body(inverse, right, parts, out):
    total = parts[0].astype(jnp.float32)
    for q in range(1, NY):
        total = total + parts[q].astype(jnp.float32)
    reduced = (right[0, 0].astype(jnp.float32) - total).astype(jnp.bfloat16)
    out[...] = jnp.dot(inverse[0, 0], reduced, preferred_element_type=jnp.float32).astype(jnp.bfloat16)


def solve_next(level, inverses, rhs, parts):
    grid_spec = pl.GridSpec(
        grid=(1,),
        in_specs=level_specs(level) + [pl.BlockSpec((NY, TILE, COLS), lambda i: (0, 0, 0))],
        out_specs=pl.BlockSpec((TILE, COLS), lambda i: (0, 0)),
    )
    return call(solve_body, block_shape(jnp.bfloat16), None, None, (inverses, rhs, parts), SOLVE_FLOPS, 8, grid_spec=grid_spec)


def accumulate(where, slots, received, level, mine, other, pieces, spots, state):
    core = where[NX]
    for piece, (base, side) in zip(pieces, spots):

        def step(j, carry, piece=piece, base=base, side=side):
            chip = (base + 2 * j) * NX + where[side]
            pair = jnp.concatenate([mine[chip, core], other[chip, core]], axis=0)
            product = jnp.dot(pair, piece[j], preferred_element_type=jnp.float32)
            state[0, slots[level, chip * NC + core]] += product[:TILE]
            state[1, received[level, chip * NC + core]] += product[TILE:]
            return carry

        lax.fori_loop(0, piece.shape[0], step, 0, unroll=4)


def early_first_body(where, slots, received, mine, other, *refs):
    pieces, state = refs[:-1], refs[-1]
    state[...] = jnp.zeros_like(state)
    accumulate(where, slots, received, 0, mine, other, pieces, NEAR_SPOTS, state)


def early_second_body(where, slots, received, mine, other, later, *refs):
    pieces, state = refs[:-1], refs[-1]
    state[...] = later[:, NY:]
    accumulate(where, slots, received, 1, mine, other, pieces, NEAR_SPOTS, state)


def early(tables, mine, other, pieces, later=None):
    operands = tables + (mine, other) + (() if later is None else (later,)) + tuple(pieces)
    return call(
        early_first_body if later is None else early_second_body,
        block_shape(jnp.float32, 2, 2 * NY if later is None else NY),
        [smem()] * 3 + [vmem()] * (len(operands) - 3),
        vmem(),
        operands,
        24 * PAIR_FLOPS,
        28,
    )


def late_body(level, where, slots, received, mine, other, state, low, high, out, near_other):
    del state
    core = where[NX]
    for piece, (base, side) in zip((low, high), FAR_SPOTS):
        for j in range(NQ):
            row = base + 2 * j
            entry = (row * NX + where[side]) * NC + core
            pair = jnp.concatenate([mine[row, 0, 0], other[row, 0, 0]], axis=0)
            product = jnp.dot(pair, piece[j], preferred_element_type=jnp.float32)
            out[0, slots[level, entry]] += product[:TILE]
            out[1, received[level, entry]] += product[TILE:]
    near_other[...] = out[1, :NY].astype(jnp.bfloat16)


def whole(shape):
    return pl.BlockSpec(shape, lambda i, where: (0,) * len(shape))


def late(level, tables, mine, other, state, pieces):
    by_place = (NQ * NP, NX, NC, TILE, TILE)
    column = pl.BlockSpec((NQ * NP, 1, 1, TILE, TILE), lambda i, where: (0, where[3], where[NX], 0, 0))
    slab = (NQ, TILE, COLS)
    grid_spec = pltpu.PrefetchScalarGridSpec(
        num_scalar_prefetch=1,
        grid=(1,),
        in_specs=[smem()] * 2 + [column] * 2 + [whole(state.shape), whole(slab), whole(slab)],
        out_specs=[whole(state.shape), whole((NY, TILE, COLS))],
    )
    return call(
        functools.partial(late_body, level),
        [jax.ShapeDtypeStruct(state.shape, jnp.float32), block_shape(jnp.bfloat16, NY)],
        None,
        None,
        tables + (mine.reshape(by_place), other.reshape(by_place), state) + tuple(pieces),
        8 * PAIR_FLOPS,
        28,
        aliases={5: 0},
        grid_spec=grid_spec,
    )


def join_body(state, received, out):
    out[...] = (state[0] + received[...].astype(jnp.float32)).astype(jnp.bfloat16)


def join(state, received):
    grid_spec = pl.GridSpec(
        grid=(1,),
        in_specs=[
            pl.BlockSpec((1, NY, TILE, COLS), lambda i: (0, 0, 0, 0)),
            pl.BlockSpec((NY, TILE, COLS), lambda i: (0, 0, 0)),
        ],
        out_specs=pl.BlockSpec((NY, TILE, COLS), lambda i: (0, 0, 0)),
    )
    return call(join_body, block_shape(jnp.bfloat16, NY), None, None, (state, received), SOLVE_FLOPS, 12, grid_spec=grid_spec)


def ring(n, d):
    return [(i, (i + d) % n) for i in range(n)]


def gather_rows(block):
    even_odd = lax.all_gather(block[None], "zq", axis=0, tiled=True)
    return lax.all_gather(even_odd[None], "zp", axis=0, tiled=True)


def gather_columns(own):
    up = functools.partial(lax.ppermute, axis_name="x", perm=ring(NX, 1))
    down = functools.partial(lax.ppermute, axis_name="x", perm=ring(NX, -1))
    low, high = own[0], own[1]
    low_left = up(low)
    high_right = down(high)
    high_left = up(high)
    low_right = down(low)
    low_far = up(low_left)
    high_far = down(high_right)
    return [low, high, low_left, high_right, high_left, low_right], [low_far, high_far]


def places():
    x = lax.axis_index("x")
    core = lax.axis_index("core")
    return jnp.stack([x, (x + NX - 1) % NX, (x + 1) % NX, (x + 2) % NX, core]).astype(jnp.int32)


def swap(value):
    return lax.ppermute(value, "core", [(0, 1), (1, 0)])


def reduce_rows(state, near_other):
    received = swap(near_other)
    return lax.all_to_all(join(state, received), "y", 0, 0, tiled=True)


def local(rhs, inverses, tiles_first, rows_first, tiles_second, rows_second):
    where = places()
    mine_first = tiles_first.reshape(CHIPS, NC, TILE, TILE)
    mine_second = tiles_second.reshape(CHIPS, NC, TILE, TILE)

    other_first = swap(mine_first)
    level_zero = solve_zero(inverses, rhs)
    near, far = gather_columns(gather_rows(level_zero))
    slots = jnp.concatenate([rows_first.reshape(1, CHIPS * NC), rows_second.reshape(1, CHIPS * NC)])
    received = swap(slots)
    tables = (where, slots, received)
    state = early(tables, mine_first, other_first, near)
    state, near_other = late(0, tables, mine_first, other_first, state, far)
    parts = reduce_rows(state, near_other)

    level_one = solve_next(1, inverses, rhs, parts)
    near, far = gather_columns(gather_rows(level_one))
    other_second = swap(mine_second)
    state = early(tables, mine_second, other_second, near, state)
    state, near_other = late(1, tables, mine_second, other_second, state, far)
    level_two = solve_next(2, inverses, rhs, reduce_rows(state, near_other))
    return jnp.stack([level_zero, level_one, level_two])[:, None]


def solution(mesh):
    grid = Mesh(mesh.devices.reshape(NQ, NP, NX, NC, NY), ("zq", "zp", "x", "core", "y"))
    blocks = ("zq", "zp", "x", "core", "y")
    rows = ("zq", "zp", "x", "core")
    in_specs = (
        P(None, blocks, None, None),
        P(None, blocks, None, None),
        P(rows, None, "y", None, None),
        P(rows, None, "y"),
        P(rows, None, "y", None, None),
        P(rows, None, "y"),
    )
    out_specs = P(None, blocks, None, None)
    return jax.shard_map(local, mesh=grid, in_specs=in_specs, out_specs=out_specs, check_vma=False)
```

```python
import functools

import jax
import jax.numpy as jnp
from jax import lax
from jax.experimental import pallas as pl
from jax.experimental.pallas import tpu as pltpu
from jax.sharding import Mesh, PartitionSpec as P


NQ, NP, NX, NC, NY = 4, 2, 4, 2, 8
TILE, COLS = 128, 384
CHIPS = NQ * NP * NX
NEAR_SPOTS = ((0, 0), (1, 0), (0, 1), (1, 2), (1, 1), (0, 2))
FAR_SPOTS = ((0, 3), (1, 3))
SOLVE_FLOPS = 2 * TILE * TILE * COLS
PAIR_FLOPS = 2 * SOLVE_FLOPS


MIB = 1 << 20


def vmem():
    return pl.BlockSpec(memory_space=pltpu.VMEM)


def smem():
    return pl.BlockSpec(memory_space=pltpu.SMEM)


def call(body, out_shape, in_specs, out_specs, operands, flops, limit, aliases=None, grid_spec=None):
    specs = {} if grid_spec is not None else {"in_specs": in_specs, "out_specs": out_specs}
    if grid_spec is not None:
        specs = {"grid_spec": grid_spec}
    return pl.pallas_call(
        body,
        out_shape=out_shape,
        input_output_aliases=aliases or {},
        compiler_params=pltpu.CompilerParams(vmem_limit_bytes=limit * MIB),
        cost_estimate=pl.CostEstimate(flops=flops, bytes_accessed=4 * MIB, transcendentals=0),
        **specs,
    )(*operands)


def block_shape(dtype, *lead):
    return jax.ShapeDtypeStruct(lead + (TILE, COLS), dtype)


def level_specs(level):
    return [
        pl.BlockSpec((1, 1, TILE, TILE), lambda i: (level, 0, 0, 0)),
        pl.BlockSpec((1, 1, TILE, COLS), lambda i: (level, 0, 0, 0)),
    ]


def solve_zero_body(inverse, right, out):
    out[...] = jnp.dot(inverse[0, 0], right[0, 0], preferred_element_type=jnp.float32).astype(jnp.bfloat16)


def solve_zero(inverses, rhs):
    grid_spec = pl.GridSpec(grid=(1,), in_specs=level_specs(0), out_specs=pl.BlockSpec((TILE, COLS), lambda i: (0, 0)))
    return call(solve_zero_body, block_shape(jnp.bfloat16), None, None, (inverses, rhs), SOLVE_FLOPS, 60, grid_spec=grid_spec)


def solve_body(inverse, right, parts, out):
    total = parts[0].astype(jnp.float32)
    for q in range(1, NY):
        total = total + parts[q].astype(jnp.float32)
    reduced = (right[0, 0].astype(jnp.float32) - total).astype(jnp.bfloat16)
    out[...] = jnp.dot(inverse[0, 0], reduced, preferred_element_type=jnp.float32).astype(jnp.bfloat16)


def solve_next(level, inverses, rhs, parts):
    grid_spec = pl.GridSpec(
        grid=(1,),
        in_specs=level_specs(level) + [pl.BlockSpec((NY, TILE, COLS), lambda i: (0, 0, 0))],
        out_specs=pl.BlockSpec((TILE, COLS), lambda i: (0, 0)),
    )
    return call(solve_body, block_shape(jnp.bfloat16), None, None, (inverses, rhs, parts), SOLVE_FLOPS, 8, grid_spec=grid_spec)


def accumulate(where, slots, received, level, mine, other, pieces, spots, state):
    core = where[NX]
    for piece, (base, side) in zip(pieces, spots):

        def step(j, carry, piece=piece, base=base, side=side):
            chip = (base + 2 * j) * NX + where[side]
            pair = jnp.concatenate([mine[chip, core], other[chip, core]], axis=0)
            product = jnp.dot(pair, piece[j], preferred_element_type=jnp.float32)
            state[0, slots[level, chip * NC + core]] += product[:TILE]
            state[1, received[level, chip * NC + core]] += product[TILE:]
            return carry

        lax.fori_loop(0, piece.shape[0], step, 0, unroll=4)


def early_first_body(where, slots, received, mine, other, *refs):
    pieces, state = refs[:-1], refs[-1]
    state[...] = jnp.zeros_like(state)
    accumulate(where, slots, received, 0, mine, other, pieces, NEAR_SPOTS, state)


def early_second_body(where, slots, received, mine, other, later, *refs):
    pieces, state = refs[:-1], refs[-1]
    state[...] = later[:, NY:]
    accumulate(where, slots, received, 1, mine, other, pieces, NEAR_SPOTS, state)


def early(tables, mine, other, pieces, later=None):
    operands = tables + (mine, other) + (() if later is None else (later,)) + tuple(pieces)
    return call(
        early_first_body if later is None else early_second_body,
        block_shape(jnp.float32, 2, 2 * NY if later is None else NY),
        [smem()] * 3 + [vmem()] * (len(operands) - 3),
        vmem(),
        operands,
        24 * PAIR_FLOPS,
        28,
    )


def late_body(level, half, where, table, tiles, state, low, high, out, *near):
    del state
    core = where[NX]
    for piece, (base, side) in zip((low, high), FAR_SPOTS):
        for j in range(NQ):
            row = base + 2 * j
            entry = (row * NX + where[side]) * NC + core
            product = jnp.dot(tiles[row, 0, 0], piece[j], preferred_element_type=jnp.float32)
            out[0, table[level, entry]] += product
    if half:
        near[0][...] = out[0, :NY].astype(jnp.bfloat16)


def whole(shape):
    return pl.BlockSpec(shape, lambda i, where: (0,) * len(shape))


def late(level, half, where, table, tiles, state, pieces):
    by_place = (NQ * NP, NX, NC, TILE, TILE)
    column = pl.BlockSpec((NQ * NP, 1, 1, TILE, TILE), lambda i, where: (0, where[3], where[NX], 0, 0))
    part = pl.BlockSpec((1,) + state.shape[1:], lambda i, where: (half, 0, 0, 0))
    slab = (NQ, TILE, COLS)
    grid_spec = pltpu.PrefetchScalarGridSpec(
        num_scalar_prefetch=1,
        grid=(1,),
        in_specs=[smem(), column, part, whole(slab), whole(slab)],
        out_specs=[part] + [whole((NY, TILE, COLS))] * half,
    )
    return call(
        functools.partial(late_body, level, half),
        [jax.ShapeDtypeStruct(state.shape, jnp.float32)] + [block_shape(jnp.bfloat16, NY)] * half,
        None,
        None,
        (where, table, tiles.reshape(by_place), state) + tuple(pieces),
        4 * PAIR_FLOPS,
        20,
        aliases={3: 0},
        grid_spec=grid_spec,
    )


def join_body(state, received, out):
    out[...] = (state[0] + received[...].astype(jnp.float32)).astype(jnp.bfloat16)


def join(state, received):
    grid_spec = pl.GridSpec(
        grid=(1,),
        in_specs=[
            pl.BlockSpec((1, NY, TILE, COLS), lambda i: (0, 0, 0, 0)),
            pl.BlockSpec((NY, TILE, COLS), lambda i: (0, 0, 0)),
        ],
        out_specs=pl.BlockSpec((NY, TILE, COLS), lambda i: (0, 0, 0)),
    )
    return call(join_body, block_shape(jnp.bfloat16, NY), None, None, (state, received), SOLVE_FLOPS, 12, grid_spec=grid_spec)


def ring(n, d):
    return [(i, (i + d) % n) for i in range(n)]


def gather_rows(block):
    even_odd = lax.all_gather(block[None], "zq", axis=0, tiled=True)
    return lax.all_gather(even_odd[None], "zp", axis=0, tiled=True)


def gather_columns(own):
    up = functools.partial(lax.ppermute, axis_name="x", perm=ring(NX, 1))
    down = functools.partial(lax.ppermute, axis_name="x", perm=ring(NX, -1))
    low, high = own[0], own[1]
    low_left = up(low)
    high_right = down(high)
    high_left = up(high)
    low_right = down(low)
    low_far = up(low_left)
    high_far = down(high_right)
    return [low, high, low_left, high_right, high_left, low_right], [low_far, high_far]


def places():
    x = lax.axis_index("x")
    core = lax.axis_index("core")
    return jnp.stack([x, (x + NX - 1) % NX, (x + 1) % NX, (x + 2) % NX, core]).astype(jnp.int32)


def swap(value):
    return lax.ppermute(value, "core", [(0, 1), (1, 0)])


def reduce_rows(level, tables, mine, other, state, pieces):
    where, slots, received = tables
    state, near_other = late(level, 1, where, received, other, state, pieces)
    near = swap(near_other)
    (state,) = late(level, 0, where, slots, mine, state, pieces)
    return state, lax.all_to_all(join(state, near), "y", 0, 0, tiled=True)


def local(rhs, inverses, tiles_first, rows_first, tiles_second, rows_second):
    where = places()
    mine_first = tiles_first.reshape(CHIPS, NC, TILE, TILE)
    mine_second = tiles_second.reshape(CHIPS, NC, TILE, TILE)

    level_zero = solve_zero(inverses, rhs)
    near, far = gather_columns(gather_rows(level_zero))
    other_first = swap(mine_first)
    slots = jnp.concatenate([rows_first.reshape(1, CHIPS * NC), rows_second.reshape(1, CHIPS * NC)])
    received = swap(slots)
    tables = (where, slots, received)
    state = early(tables, mine_first, other_first, near)
    state, parts = reduce_rows(0, tables, mine_first, other_first, state, far)

    level_one = solve_next(1, inverses, rhs, parts)
    near, far = gather_columns(gather_rows(level_one))
    other_second = swap(mine_second)
    state = early(tables, mine_second, other_second, near, state)
    state, parts = reduce_rows(1, tables, mine_second, other_second, state, far)
    level_two = solve_next(2, inverses, rhs, parts)
    return jnp.stack([level_zero, level_one, level_two])[:, None]


def solution(mesh):
    grid = Mesh(mesh.devices.reshape(NQ, NP, NX, NC, NY), ("zq", "zp", "x", "core", "y"))
    blocks = ("zq", "zp", "x", "core", "y")
    rows = ("zq", "zp", "x", "core")
    in_specs = (
        P(None, blocks, None, None),
        P(None, blocks, None, None),
        P(rows, None, "y", None, None),
        P(rows, None, "y"),
        P(rows, None, "y", None, None),
        P(rows, None, "y"),
    )
    out_specs = P(None, blocks, None, None)
    return jax.shard_map(local, mesh=grid, in_specs=in_specs, out_specs=out_specs, check_vma=False)
```

```python
import functools

import jax
import jax.numpy as jnp
from jax import lax
from jax.experimental import pallas as pl
from jax.experimental.pallas import tpu as pltpu
from jax.sharding import Mesh, PartitionSpec as P


NQ, NP, NX, NC, NY = 4, 2, 4, 2, 8
TILE, COLS = 128, 384
CHIPS = NQ * NP * NX
LOW = 5
ROWS = NQ * NP
NEAR_SPOTS = ((0, 0), (LOW, 0), (0, 1), (LOW, 2), (LOW, 1), (0, 2))
FAR_SPOTS = ((0, 3), (LOW, 3))
SOLVE_FLOPS = 2 * TILE * TILE * COLS
PAIR_FLOPS = 2 * SOLVE_FLOPS


MIB = 1 << 20


def vmem():
    return pl.BlockSpec(memory_space=pltpu.VMEM)


def smem():
    return pl.BlockSpec(memory_space=pltpu.SMEM)


def call(body, out_shape, in_specs, out_specs, operands, flops, limit, aliases=None, grid_spec=None):
    specs = {} if grid_spec is not None else {"in_specs": in_specs, "out_specs": out_specs}
    if grid_spec is not None:
        specs = {"grid_spec": grid_spec}
    return pl.pallas_call(
        body,
        out_shape=out_shape,
        input_output_aliases=aliases or {},
        compiler_params=pltpu.CompilerParams(vmem_limit_bytes=limit * MIB),
        cost_estimate=pl.CostEstimate(flops=flops, bytes_accessed=4 * MIB, transcendentals=0),
        **specs,
    )(*operands)


def block_shape(dtype, *lead):
    return jax.ShapeDtypeStruct(lead + (TILE, COLS), dtype)


def level_specs(level):
    return [
        pl.BlockSpec((1, 1, TILE, TILE), lambda i: (level, 0, 0, 0)),
        pl.BlockSpec((1, 1, TILE, COLS), lambda i: (level, 0, 0, 0)),
    ]


def solve_zero_body(inverse, right, out):
    out[...] = jnp.dot(inverse[0, 0], right[0, 0], preferred_element_type=jnp.float32).astype(jnp.bfloat16)


def solve_zero(inverses, rhs):
    grid_spec = pl.GridSpec(grid=(1,), in_specs=level_specs(0), out_specs=pl.BlockSpec((TILE, COLS), lambda i: (0, 0)))
    return call(solve_zero_body, block_shape(jnp.bfloat16), None, None, (inverses, rhs), SOLVE_FLOPS, 60, grid_spec=grid_spec)


def solve_body(inverse, right, parts, out):
    total = parts[0].astype(jnp.float32)
    for q in range(1, NY):
        total = total + parts[q].astype(jnp.float32)
    reduced = (right[0, 0].astype(jnp.float32) - total).astype(jnp.bfloat16)
    out[...] = jnp.dot(inverse[0, 0], reduced, preferred_element_type=jnp.float32).astype(jnp.bfloat16)


def solve_next(level, inverses, rhs, parts):
    grid_spec = pl.GridSpec(
        grid=(1,),
        in_specs=level_specs(level) + [pl.BlockSpec((NY, TILE, COLS), lambda i: (0, 0, 0))],
        out_specs=pl.BlockSpec((TILE, COLS), lambda i: (0, 0)),
    )
    return call(solve_body, block_shape(jnp.bfloat16), None, None, (inverses, rhs, parts), SOLVE_FLOPS, 8, grid_spec=grid_spec)


def accumulate(where, slots, received, level, mine, other, pieces, spots, state):
    core = where[NX]
    for piece, (base, side) in zip(pieces, spots):

        def step(j, carry, piece=piece, base=base, side=side):
            k = base + j
            chip = (2 * lax.rem(k, NQ) + lax.div(k, NQ)) * NX + where[side]
            pair = jnp.concatenate([mine[chip, core], other[chip, core]], axis=0)
            product = jnp.dot(pair, piece[j], preferred_element_type=jnp.float32)
            state[0, slots[level, chip * NC + core]] += product[:TILE]
            state[1, received[level, chip * NC + core]] += product[TILE:]
            return carry

        lax.fori_loop(0, piece.shape[0], step, 0, unroll=True)


def early_first_body(where, slots, received, mine, other, *refs):
    pieces, state = refs[:-1], refs[-1]
    state[...] = jnp.zeros_like(state)
    accumulate(where, slots, received, 0, mine, other, pieces, NEAR_SPOTS, state)


def early_second_body(where, slots, received, mine, other, later, *refs):
    pieces, state = refs[:-1], refs[-1]
    state[...] = later[:, NY:]
    accumulate(where, slots, received, 1, mine, other, pieces, NEAR_SPOTS, state)


def early(tables, mine, other, pieces, later=None):
    operands = tables + (mine, other) + (() if later is None else (later,)) + tuple(pieces)
    return call(
        early_first_body if later is None else early_second_body,
        block_shape(jnp.float32, 2, 2 * NY if later is None else NY),
        [smem()] * 3 + [vmem()] * (len(operands) - 3),
        vmem(),
        operands,
        24 * PAIR_FLOPS,
        28,
    )


def late_body(level, half, where, table, tiles, state, low, high, out, *near):
    del state
    core = where[NX]
    for piece, (base, side) in zip((low, high), FAR_SPOTS):
        for j in range(piece.shape[0]):
            row = 2 * ((base + j) % NQ) + (base + j) // NQ
            entry = (row * NX + where[side]) * NC + core
            product = jnp.dot(tiles[row, 0, 0], piece[j], preferred_element_type=jnp.float32)
            out[0, table[level, entry]] += product
    if half:
        near[0][...] = out[0, :NY].astype(jnp.bfloat16)


def whole(shape):
    return pl.BlockSpec(shape, lambda i, where: (0,) * len(shape))


def late(level, half, where, table, tiles, state, pieces):
    by_place = (ROWS, NX, NC, TILE, TILE)
    column = pl.BlockSpec((ROWS, 1, 1, TILE, TILE), lambda i, where: (0, where[3], where[NX], 0, 0))
    part = pl.BlockSpec((1,) + state.shape[1:], lambda i, where: (half, 0, 0, 0))
    grid_spec = pltpu.PrefetchScalarGridSpec(
        num_scalar_prefetch=1,
        grid=(1,),
        in_specs=[smem(), column, part] + [whole(piece.shape) for piece in pieces],
        out_specs=[part] + [whole((NY, TILE, COLS))] * half,
    )
    return call(
        functools.partial(late_body, level, half),
        [jax.ShapeDtypeStruct(state.shape, jnp.float32)] + [block_shape(jnp.bfloat16, NY)] * half,
        None,
        None,
        (where, table, tiles.reshape(by_place), state) + tuple(pieces),
        4 * PAIR_FLOPS,
        20,
        aliases={3: 0},
        grid_spec=grid_spec,
    )


def join_body(state, received, out):
    out[...] = (state[0] + received[...].astype(jnp.float32)).astype(jnp.bfloat16)


def join(state, received):
    grid_spec = pl.GridSpec(
        grid=(1,),
        in_specs=[
            pl.BlockSpec((1, NY, TILE, COLS), lambda i: (0, 0, 0, 0)),
            pl.BlockSpec((NY, TILE, COLS), lambda i: (0, 0, 0)),
        ],
        out_specs=pl.BlockSpec((NY, TILE, COLS), lambda i: (0, 0, 0)),
    )
    return call(join_body, block_shape(jnp.bfloat16, NY), None, None, (state, received), SOLVE_FLOPS, 12, grid_spec=grid_spec)


def ring(n, d):
    return [(i, (i + d) % n) for i in range(n)]


def gather_rows(block):
    even_odd = lax.all_gather(block[None], "zq", axis=0, tiled=True)
    return lax.all_gather(even_odd, "zp", axis=0, tiled=True)


def gather_columns(own):
    up = functools.partial(lax.ppermute, axis_name="x", perm=ring(NX, 1))
    down = functools.partial(lax.ppermute, axis_name="x", perm=ring(NX, -1))
    low, high = own[:LOW], own[LOW:]
    low_left = up(low)
    high_right = down(high)
    high_left = up(high)
    low_right = down(low)
    low_far = up(low_left)
    high_far = down(high_right)
    return [low, high, low_left, high_right, high_left, low_right], [low_far, high_far]


def places():
    x = lax.axis_index("x")
    core = lax.axis_index("core")
    return jnp.stack([x, (x + NX - 1) % NX, (x + 1) % NX, (x + 2) % NX, core]).astype(jnp.int32)


def swap(value):
    return lax.ppermute(value, "core", [(0, 1), (1, 0)])


def reduce_rows(level, tables, mine, other, state, pieces):
    where, slots, received = tables
    state, near_other = late(level, 1, where, received, other, state, pieces)
    near = swap(near_other)
    (state,) = late(level, 0, where, slots, mine, state, pieces)
    return state, lax.all_to_all(join(state, near), "y", 0, 0, tiled=True)


def local(rhs, inverses, tiles_first, rows_first, tiles_second, rows_second):
    where = places()
    mine_first = tiles_first.reshape(CHIPS, NC, TILE, TILE)
    mine_second = tiles_second.reshape(CHIPS, NC, TILE, TILE)

    level_zero = solve_zero(inverses, rhs)
    near, far = gather_columns(gather_rows(level_zero))
    other_first = swap(mine_first)
    slots = jnp.concatenate([rows_first.reshape(1, CHIPS * NC), rows_second.reshape(1, CHIPS * NC)])
    received = swap(slots)
    tables = (where, slots, received)
    state = early(tables, mine_first, other_first, near)
    state, parts = reduce_rows(0, tables, mine_first, other_first, state, far)

    level_one = solve_next(1, inverses, rhs, parts)
    near, far = gather_columns(gather_rows(level_one))
    other_second = swap(mine_second)
    state = early(tables, mine_second, other_second, near, state)
    state, parts = reduce_rows(1, tables, mine_second, other_second, state, far)
    level_two = solve_next(2, inverses, rhs, parts)
    return jnp.stack([level_zero, level_one, level_two])[:, None]


def solution(mesh):
    grid = Mesh(mesh.devices.reshape(NQ, NP, NX, NC, NY), ("zq", "zp", "x", "core", "y"))
    blocks = ("zq", "zp", "x", "core", "y")
    rows = ("zq", "zp", "x", "core")
    in_specs = (
        P(None, blocks, None, None),
        P(None, blocks, None, None),
        P(rows, None, "y", None, None),
        P(rows, None, "y"),
        P(rows, None, "y", None, None),
        P(rows, None, "y"),
    )
    out_specs = P(None, blocks, None, None)
    return jax.shard_map(local, mesh=grid, in_specs=in_specs, out_specs=out_specs, check_vma=False)
```
